16 devices in a mesh: dp: 4 (over z, y), tp: 4 (over x, core).
Axes of the slice: x: 2, y: 2, z: 2, core: 2. Of those that a mesh axis runs over, the one named last changes fastest.
Arguments:
- x_in: bfloat16 [512, 1024], P('dp'), parts along dimension 0
- seq_lens: int32 [512], P('dp'), parts along dimension 0
- g_attn: bfloat16 [2, 1024], replicated
- g_mlp: bfloat16 [2, 1024], replicated
- w_q: bfloat16 [2, 1024, 2048], P(None, None, 'tp')
- b_q: bfloat16 [2, 2048], P(None, 'tp')
- w_k: bfloat16 [2, 1024, 1024], P(None, None, 'tp')
- b_k: bfloat16 [2, 1024], P(None, 'tp')
- w_v: bfloat16 [2, 1024, 1024], P(None, None, 'tp')
- b_v: bfloat16 [2, 1024], P(None, 'tp')
- w_o: bfloat16 [2, 2048, 1024], P(None, 'tp')
- w_gate: bfloat16 [2, 1024, 3072], P(None, None, 'tp')
- w_up: bfloat16 [2, 1024, 3072], P(None, None, 'tp')
- w_down: bfloat16 [2, 3072, 1024], P(None, 'tp')
- k_cache: bfloat16 [2, 512, 128, 8, 128], P(None, 'dp', None, 'tp'), parts along dimension 1
- v_cache: bfloat16 [2, 512, 128, 8, 128], P(None, 'dp', None, 'tp'), parts along dimension 1
Outputs:
- output 1: bfloat16 [512, 1024], P('dp'), parts along dimension 0
- output 2: bfloat16 [2, 512, 128, 8, 128], P(None, 'dp', None, 'tp'), parts along dimension 1
- output 3: bfloat16 [2, 512, 128, 8, 128], P(None, 'dp', None, 'tp'), parts along dimension 1
There are 4 independent parts. The reference program is written for one: setup_inputs(seed, part) draws one part's arguments, and reference() takes and returns one part's arrays. A program takes and returns all parts, laid end to end along the dimension named above; an argument that names none is the same for every part.
All inputs are finite; a program needn't handle non-finite values.
Results may differ from the reference program's by a relative error of at most 0.0187495.
Values are sent between devices in bfloat16 or wider.
A program may use at most 1 GiB of HBM per device.

```python
import math
import jax
import jax.numpy as jnp
from jax import lax

D = 1024
HEADS = 16
KV_HEADS = 8
HEAD = 128
FF = 3072
BATCH = 128
CACHE = 128
LAYERS = 2
ROPE_THETA = 1000000.0
EPS = 1e-6


def setup_inputs(seed: int = 0, part: int = 0) -> dict:
    root_key = jax.random.key(seed)
    weight_keys = jax.random.split(root_key, 12)
    part_keys = jax.random.split(jax.random.fold_in(root_key, part), 5)
    group_size = HEADS // KV_HEADS
    q_width = HEADS * HEAD
    kv_width = KV_HEADS * HEAD
    couple = 0.6 * math.log(CACHE) / math.sqrt(HEAD)

    def normal(sub_key, arr_shape, arr_scale):
        return jax.random.normal(sub_key, arr_shape, jnp.float32) * arr_scale

    seq_lens = jax.random.randint(part_keys[1], (BATCH,), CACHE // 16, CACHE, dtype=jnp.int32)
    seq_lens = seq_lens.at[0].set(CACHE - 1).at[1].set(CACHE // 16)
    k_bias = normal(weight_keys[5], (LAYERS, KV_HEADS, 1, HEAD), 1.0)
    q_bias = couple * k_bias + normal(weight_keys[3], (LAYERS, KV_HEADS, group_size, HEAD), 1.0)
    cache_shape = (LAYERS, BATCH, CACHE, KV_HEADS, HEAD)
    v_mean = normal(part_keys[3], (LAYERS, BATCH, 1, KV_HEADS, HEAD), 1.0)
    return {
        "x_in": normal(part_keys[0], (BATCH, D), 1.0).astype(jnp.bfloat16),
        "seq_lens": seq_lens,
        "g_attn": (1.0 + normal(weight_keys[0], (LAYERS, D), 0.25)).astype(jnp.bfloat16),
        "g_mlp": (1.0 + normal(weight_keys[1], (LAYERS, D), 0.25)).astype(jnp.bfloat16),
        "w_q": normal(weight_keys[2], (LAYERS, D, q_width), D ** -0.5).astype(jnp.bfloat16),
        "b_q": q_bias.reshape(LAYERS, q_width).astype(jnp.bfloat16),
        "w_k": normal(weight_keys[4], (LAYERS, D, kv_width), D ** -0.5).astype(jnp.bfloat16),
        "b_k": k_bias.reshape(LAYERS, kv_width).astype(jnp.bfloat16),
        "w_v": normal(weight_keys[6], (LAYERS, D, kv_width), D ** -0.5).astype(jnp.bfloat16),
        "b_v": normal(weight_keys[7], (LAYERS, kv_width), 1.0).astype(jnp.bfloat16),
        "w_o": normal(weight_keys[8], (LAYERS, q_width, D), q_width ** -0.5).astype(jnp.bfloat16),
        "w_gate": normal(weight_keys[9], (LAYERS, D, FF), D ** -0.5).astype(jnp.bfloat16),
        "w_up": normal(weight_keys[10], (LAYERS, D, FF), D ** -0.5).astype(jnp.bfloat16),
        "w_down": normal(weight_keys[11], (LAYERS, FF, D), FF ** -0.5).astype(jnp.bfloat16),
        "k_cache": normal(part_keys[2], cache_shape, 1.0).astype(jnp.bfloat16),
        "v_cache": (v_mean + normal(part_keys[4], cache_shape, 1.0)).astype(jnp.bfloat16),
    }


def rms_norm(vec_in, gain_vec):
    vec_f32 = vec_in.astype(jnp.float32)
    mean_sq = jnp.mean(vec_f32 * vec_f32, axis=-1, keepdims=True)
    return (vec_f32 * lax.rsqrt(mean_sq + EPS) * gain_vec.astype(jnp.float32)).astype(jnp.bfloat16)


def rope_tables(seq_lens, head_dim):
    half_dim = head_dim // 2
    inv_freq = ROPE_THETA ** (-2.0 * jnp.arange(half_dim, dtype=jnp.float32) / head_dim)
    angles = seq_lens.astype(jnp.float32)[:, None] * inv_freq[None, :]
    angles = jnp.concatenate([angles, angles], axis=-1)[:, None, :]
    return jnp.cos(angles), jnp.sin(angles)


def apply_rope(vec_in, cos_tab, sin_tab):
    half_dim = vec_in.shape[-1] // 2
    rotated = jnp.concatenate([-vec_in[..., half_dim:], vec_in[..., :half_dim]], axis=-1)
    return vec_in * cos_tab + rotated * sin_tab


def decoder_layer(x_in, seq_lens, cos_tab, sin_tab, params):
    g_attn, g_mlp, w_q, b_q, w_k, b_k, w_v, b_v, w_o, w_gate, w_up, w_down, k_cache, v_cache = params
    num_rows = x_in.shape[0]
    group_size = HEADS // KV_HEADS
    normed = rms_norm(x_in, g_attn)
    q_full = jnp.dot(normed, w_q, preferred_element_type=jnp.float32) + b_q.astype(jnp.float32)
    q_rot = apply_rope(q_full.reshape(num_rows, HEADS, HEAD), cos_tab, sin_tab).astype(jnp.bfloat16)
    k_full = jnp.dot(normed, w_k, preferred_element_type=jnp.float32) + b_k.astype(jnp.float32)
    k_rot = apply_rope(k_full.reshape(num_rows, KV_HEADS, HEAD), cos_tab, sin_tab).astype(jnp.bfloat16)
    v_full = jnp.dot(normed, w_v, preferred_element_type=jnp.float32) + b_v.astype(jnp.float32)
    v_new = v_full.astype(jnp.bfloat16).reshape(num_rows, KV_HEADS, HEAD)
    slot_ids = jnp.arange(CACHE, dtype=jnp.int32)
    is_new = (slot_ids[None, :] == seq_lens[:, None])[:, :, None, None]
    k_next = jnp.where(is_new, k_rot[:, None], k_cache)
    v_next = jnp.where(is_new, v_new[:, None], v_cache)
    q_grouped = q_rot.reshape(num_rows, KV_HEADS, group_size, HEAD)

    def attend_row(row_args):
        q_row, k_row, v_row, row_len = row_args
        scores = jnp.einsum("kgd,skd->kgs", q_row.astype(jnp.float32), k_row.astype(jnp.float32)) * (HEAD ** -0.5)
        visible = slot_ids <= row_len
        scores = jnp.where(visible[None, None, :], scores, -1e30)
        attn_probs = jax.nn.softmax(scores, axis=-1).astype(jnp.bfloat16)
        out_row = jnp.einsum("kgs,skd->kgd", attn_probs.astype(jnp.float32), v_row.astype(jnp.float32))
        return out_row.astype(jnp.bfloat16)

    attn_out = lax.map(attend_row, (q_grouped, k_next, v_next, seq_lens)).reshape(num_rows, HEADS * HEAD)
    x_mid = (x_in.astype(jnp.float32) + jnp.dot(attn_out, w_o, preferred_element_type=jnp.float32)).astype(jnp.bfloat16)
    normed_mlp = rms_norm(x_mid, g_mlp)
    gate_proj = jnp.dot(normed_mlp, w_gate, preferred_element_type=jnp.float32)
    up_proj = jnp.dot(normed_mlp, w_up, preferred_element_type=jnp.float32)
    hidden_act = (jax.nn.silu(gate_proj) * up_proj).astype(jnp.bfloat16)
    x_next = (x_mid.astype(jnp.float32) + jnp.dot(hidden_act, w_down, preferred_element_type=jnp.float32)).astype(jnp.bfloat16)
    return x_next, k_next, v_next


def reference(x_in, seq_lens, g_attn, g_mlp, w_q, b_q, w_k, b_k, w_v, b_v, w_o, w_gate, w_up, w_down, k_cache, v_cache):
    cos_tab, sin_tab = rope_tables(seq_lens, HEAD)

    def layer_step(x_carry, params):
        x_next, k_next, v_next = decoder_layer(x_carry, seq_lens, cos_tab, sin_tab, params)
        return x_next, (k_next, v_next)

    layer_params = (g_attn, g_mlp, w_q, b_q, w_k, b_k, w_v, b_v, w_o, w_gate, w_up, w_down, k_cache, v_cache)
    x_out, cache_pair = lax.scan(layer_step, x_in, layer_params)
    return x_out, cache_pair[0], cache_pair[1]
```

```python
import functools

import jax
import jax.numpy as jnp
import numpy as np
from jax import lax
from jax.experimental import pallas as pl
from jax.experimental.pallas import tpu as pltpu
from jax.sharding import PartitionSpec as P

ROPE_THETA = 1000000.0
EPS = 1e-6
F32 = jnp.float32
BF16 = jnp.bfloat16
MESH = pl.DeviceIdType.MESH
BLK = 8


def dot(lhs, rhs):
    return jnp.dot(lhs, rhs, preferred_element_type=F32)


def dot_nt(lhs, rhs):
    return lax.dot_general(lhs, rhs, (((1,), (1,)), ((), ())), preferred_element_type=F32)


def one_hot(shape, hit):
    rows = lax.broadcasted_iota(jnp.int32, shape, 0)
    cols = lax.broadcasted_iota(jnp.int32, shape, 1)
    return jnp.where(hit(rows, cols), 1.0, 0.0).astype(BF16)


def step_kernel(chunk, x_ref, lens_ref, freq_ref, g_attn_ref, g_mlp_ref, bq_ref, bk_ref, bv_ref,
                wq_hbm, wk_hbm, wv_hbm, wo_hbm, wg_hbm, wu_hbm, wd_hbm, kc_hbm, vc_hbm,
                xo_ref, ko_ref, vo_ref,
                wq, wk, wv, wo, wg, wu, wd,
                spread, gather, ungather, kpat, vpat, qlhs, scores, rows_out, limit, ppat, cos_t, sin_t,
                part, recv_a, mid, recv_b, xs,
                w_sem, k_sem, v_sem, send_sem, recv_sem):
    layers, batch, slots2, head = ko_ref.shape
    heads = wq.shape[2] // head
    kv = wk.shape[2] // head
    group = heads // kv
    n_chunks = batch // chunk
    half = chunk // 2
    blocks = chunk // BLK
    tp = lax.axis_index("tp")
    core = lax.rem(tp, 2)
    chip = tp // 2
    core_peer = {"tp": chip * 2 + (1 - core)}
    chip_peer = {"tp": (1 - chip) * 2 + core}

    weights = ((wq_hbm, wq), (wk_hbm, wk), (wv_hbm, wv), (wo_hbm, wo), (wg_hbm, wg), (wu_hbm, wu), (wd_hbm, wd))

    def weight_copy(layer, idx):
        src, dst = weights[idx]
        return pltpu.make_async_copy(src.at[layer], dst.at[layer], w_sem.at[layer, idx])

    def cache_copy(src, dst, sem, layer, blk):
        return pltpu.make_async_copy(src.at[layer, pl.ds(blk * BLK, BLK)], dst.at[layer, pl.ds(blk * BLK, BLK)], sem.at[layer, blk])

    def start_weights(layer, idxs):
        for idx in idxs:
            weight_copy(layer, idx).start()

    def wait_weights(layer, idxs):
        for idx in idxs:
            weight_copy(layer, idx).wait()

    def start_cache(layer, c):
        for src, dst, sem in ((kc_hbm, ko_ref, k_sem), (vc_hbm, vo_ref, v_sem)):
            @pl.loop(0, blocks)
            def _(i):
                cache_copy(src, dst, sem, layer, c * blocks + i).start()

    start_weights(0, (0, 1, 2))
    start_cache(0, 0)

    barrier = pltpu.get_barrier_semaphore()
    for peer in (core_peer, chip_peer):
        pl.semaphore_signal(barrier, inc=1, device_id=peer, device_id_type=MESH)
    pl.semaphore_wait(barrier, 2)

    spread[...] = one_hot(spread.shape, lambda r, c: c == (r % kv) * chunk + r // 16)
    gather[...] = one_hot(gather.shape, lambda r, c: c == (r % heads) * chunk + r // heads)
    ungather[...] = one_hot(ungather.shape, lambda r, c: r == (c % heads) * chunk + c // heads)
    lens = lens_ref[...].astype(F32)
    sq = (batch, batch)
    diag = lax.broadcasted_iota(jnp.int32, sq, 0) == lax.broadcasted_iota(jnp.int32, sq, 1)
    len_col = jnp.sum(jnp.where(diag, jnp.broadcast_to(lens, sq), 0.0), axis=1, keepdims=True)
    len_cols = jnp.broadcast_to(len_col, (batch, head))
    angles = len_cols * freq_ref[...]
    cos_t[...] = jnp.cos(angles)
    lane = lax.broadcasted_iota(jnp.int32, (batch, head), 1)
    sine = jnp.sin(angles)
    sin_t[...] = jnp.where(lane < head // 2, -sine, sine)
    len_bf = len_cols.astype(BF16)
    ppat[...] = dot(one_hot((batch * 16, batch), lambda r, c: c == r // 16), len_bf).astype(BF16)
    row_len = dot(one_hot((batch * heads, batch), lambda r, c: c == r // heads), len_bf)
    row_len = jnp.concatenate([row_len] * (slots2 // head), axis=1)
    lim_shape = (batch * heads, slots2)
    q_head = lax.broadcasted_iota(jnp.int32, lim_shape, 0) % heads
    own = lax.broadcasted_iota(jnp.int32, lim_shape, 1) % kv == q_head // group
    limit[...] = jnp.where(own, row_len, -1.0)
    slot_of = (lax.broadcasted_iota(jnp.int32, (16, head), 0) // kv).astype(F32).astype(BF16)

    def rms_norm(x_bf, gain_ref, layer):
        x = x_bf.astype(F32)
        mean_sq = jnp.mean(x * x, axis=-1, keepdims=True)
        return (x * lax.rsqrt(mean_sq + EPS) * gain_ref[pl.ds(layer, 1), :].astype(F32)).astype(BF16)

    def read_x(stage, c):
        src = x_ref if stage == 0 else xs.at[stage - 1]
        return src[pl.ds(c * chunk, chunk), :]

    def qkv(layer, c):
        h = rms_norm(read_x(2 * layer, c), g_attn_ref, layer)
        cos = cos_t[pl.ds(c * chunk, chunk), :]
        sin = sin_t[pl.ds(c * chunk, chunk), :]

        def rope(vec):
            return (vec * cos + pltpu.roll(vec, head // 2, 1) * sin).astype(BF16)

        def split(mat, n):
            return [mat[:, i * head:(i + 1) * head] for i in range(n)]

        q = dot(h, wq[layer]) + bq_ref[pl.ds(layer, 1), :].astype(F32)
        k = dot(h, wk[layer]) + bk_ref[pl.ds(layer, 1), :].astype(F32)
        v = dot(h, wv[layer]) + bv_ref[pl.ds(layer, 1), :].astype(F32)
        q_stack = jnp.concatenate([rope(m) for m in split(q, heads)], axis=0)
        k_stack = jnp.concatenate([rope(m) for m in split(k, kv)], axis=0)
        v_stack = jnp.concatenate([m.astype(BF16) for m in split(v, kv)], axis=0)
        kpat[...] = dot(spread[...], k_stack).astype(BF16)
        vpat[...] = dot(spread[...], v_stack).astype(BF16)
        q_rows = dot(gather[...], q_stack)
        first = lax.broadcasted_iota(jnp.int32, q_rows.shape, 0) % (2 * heads) < heads
        qlhs[...] = jnp.concatenate([jnp.where(first, q_rows, 0.0), jnp.where(first, 0.0, q_rows)], axis=1)

    def update(out_ref, pat_ref, layer, c, b):
        row = c * chunk + b
        old = out_ref[layer, row]
        pat = pat_ref[pl.ds(pl.multiple_of(b * 16, 16), 16), :]
        p = ppat[pl.ds(pl.multiple_of(row * 16, 16), 16), :]
        tiles = []
        for t in range(slots2 // 16):
            here = slot_of == p - jnp.asarray(t * (16 // kv), BF16)
            tiles.append(jnp.where(here, pat, old[t * 16:(t + 1) * 16, :]))
        new = jnp.concatenate(tiles, axis=0)
        out_ref[layer, row] = new
        return new

    def attn_scores(layer, c):
        @pl.loop(0, blocks)
        def _(i):
            cache_copy(kc_hbm, ko_ref, k_sem, layer, c * blocks + i).wait()
            for pair in range(BLK // 2):
                b = i * BLK + 2 * pair
                rhs = jnp.concatenate([update(ko_ref, kpat, layer, c, b), update(ko_ref, kpat, layer, c, b + 1)], axis=1)
                rows = pl.ds(pl.multiple_of(b * heads, 2 * heads), 2 * heads)
                scores[rows, :] = dot_nt(qlhs[rows, :].astype(BF16), rhs)

    def attn_softmax(c):
        s = scores[...] * (head ** -0.5)
        slot = (lax.broadcasted_iota(jnp.int32, s.shape, 1) // kv).astype(F32)
        s = jnp.where(slot <= limit[pl.ds(c * chunk * heads, chunk * heads), :], s, -1e30)
        e = jnp.exp(s - jnp.max(s, axis=-1, keepdims=True))
        scores[...] = e / jnp.sum(e, axis=-1, keepdims=True)

    def attn_values(layer, c):
        @pl.loop(0, blocks)
        def _(i):
            cache_copy(vc_hbm, vo_ref, v_sem, layer, c * blocks + i).wait()
            for pair in range(BLK // 2):
                b = i * BLK + 2 * pair
                rhs = jnp.concatenate([update(vo_ref, vpat, layer, c, b), update(vo_ref, vpat, layer, c, b + 1)], axis=1)
                rows = pl.ds(pl.multiple_of(b * heads, 2 * heads), 2 * heads)
                out = dot(scores[rows, :].astype(BF16), rhs)
                first = lax.broadcasted_iota(jnp.int32, (2 * heads, head), 0) < heads
                rows_out[rows, :] = jnp.where(first, out[:, :head], out[:, head:])

    def attn_project(layer, c):
        stacked = dot(ungather[...], rows_out[...].astype(BF16)).astype(BF16)
        attn = jnp.concatenate([stacked[i * chunk:(i + 1) * chunk, :] for i in range(heads)], axis=1)
        part[2 * layer * n_chunks + c] = dot(attn, wo[layer]).astype(BF16)

    def mlp(layer, c):
        h = rms_norm(read_x(2 * layer + 1, c), g_mlp_ref, layer)
        act = (jax.nn.silu(dot(h, wg[layer])) * dot(h, wu[layer])).astype(BF16)
        part[(2 * layer + 1) * n_chunks + c] = dot(act, wd[layer]).astype(BF16)

    mine = pl.ds(pl.multiple_of(core * half, half), half)
    other = pl.ds(pl.multiple_of((1 - core) * half, half), half)

    def send(hop, inst, src, dst, peer):
        return pltpu.make_async_remote_copy(src_ref=src, dst_ref=dst, send_sem=send_sem.at[hop, inst], recv_sem=recv_sem.at[hop, inst],
                                            device_id=peer, device_id_type=MESH)

    def hop_a(s, c):
        inst = s * n_chunks + c
        return send(0, inst, part.at[inst, other], recv_a.at[inst], core_peer)

    def hop_b(s, c):
        inst = s * n_chunks + c
        return send(1, inst, mid.at[inst], recv_b.at[inst], chip_peer)

    def hop_c(s, c):
        rows = pl.ds(pl.multiple_of(c * chunk + core * half, half), half)
        return send(2, s * n_chunks + c, xs.at[s, rows], xs.at[s, rows], core_peer)

    def sum_start(s, c):
        hop_a(s, c).start()

    def sum_cross(s, c):
        inst = s * n_chunks + c
        hop_a(s, c).wait_recv()
        mid[inst] = (part[inst, mine, :].astype(F32) + recv_a[inst].astype(F32)).astype(BF16)
        hop_b(s, c).start()

    def sum_share(s, c):
        inst = s * n_chunks + c
        hop_b(s, c).wait_recv()
        rows = pl.ds(pl.multiple_of(c * chunk + core * half, half), half)
        before = (x_ref if s == 0 else xs.at[s - 1])[rows, :]
        total = mid[inst].astype(F32) + recv_b[inst].astype(F32)
        xs[s, rows, :] = (before.astype(F32) + total).astype(BF16)
        hop_c(s, c).start()

    def sum_end(s, c):
        hop_c(s, c).wait_recv()

    def attention(layer, c, between=None):
        qkv(layer, c)
        attn_scores(layer, c)
        if between is not None:
            between()
        attn_softmax(c)
        attn_values(layer, c)
        attn_project(layer, c)
        sum_start(2 * layer, c)

    for layer in range(layers):
        s = 2 * layer
        if layer == 0:
            wait_weights(0, (0, 1, 2))
            start_weights(0, (3,))
            start_cache(0, 1)
            qkv(0, 0)
        else:
            wait_weights(layer, (0, 1, 2))
            sum_end(s - 1, 0)
            qkv(layer, 0)
        attn_scores(layer, 0)
        if layer > 0:
            sum_share(s - 1, 1)
        attn_softmax(0)
        attn_values(layer, 0)
        wait_weights(layer, (3,))
        attn_project(layer, 0)
        sum_start(s, 0)
        if layer == 0:
            start_weights(0, (4, 5, 6))
            start_weights(1, (0, 1, 2))
            start_cache(1, 0)
        else:
            sum_end(s - 1, 1)
        qkv(layer, 1)
        sum_cross(s, 0)
        attn_scores(layer, 1)
        attn_softmax(1)
        attn_values(layer, 1)
        attn_project(layer, 1)
        sum_start(s, 1)
        if layer == 0:
            start_cache(1, 1)
            start_weights(1, (3, 4, 5, 6))
        sum_share(s, 0)
        sum_cross(s, 1)
        wait_weights(layer, (4, 5, 6))
        sum_end(s, 0)
        mlp(layer, 0)
        sum_start(s + 1, 0)
        sum_share(s, 1)
        sum_cross(s + 1, 0)
        sum_end(s, 1)
        mlp(layer, 1)
        sum_start(s + 1, 1)
        sum_cross(s + 1, 1)
        sum_share(s + 1, 0)
        if layer == layers - 1:
            sum_end(s + 1, 0)
            sum_share(s + 1, 1)
            sum_end(s + 1, 1)

    for s in range(2 * layers):
        for c in range(n_chunks):
            hop_a(s, c).wait_send()
            hop_b(s, c).wait_send()
            hop_c(s, c).wait_send()
    xo_ref[...] = xs[2 * layers - 1]


def run_step(x_in, seq_lens, g_attn, g_mlp, w_q, b_q, w_k, b_k, w_v, b_v, w_o, w_gate, w_up, w_down, k_cache, v_cache):
    layers, batch, slots, kv, head = k_cache.shape
    width = x_in.shape[1]
    heads = w_q.shape[2] // head
    chunk = batch // 2
    flat = (layers, batch, slots * kv, head)
    exponent = -2.0 * (np.arange(head) % (head // 2)) / head
    freq = jnp.asarray((ROPE_THETA ** exponent)[None, :], F32)
    insts = 2 * layers * 2
    vmem = pl.BlockSpec(memory_space=pltpu.VMEM)
    hbm = pl.BlockSpec(memory_space=pl.ANY)
    weights = (w_q, w_k, w_v, w_o, w_gate, w_up, w_down)
    scratch = [pltpu.VMEM(w.shape, BF16) for w in weights]
    scratch += [
        pltpu.VMEM((chunk * 16, kv * chunk), BF16),
        pltpu.VMEM((chunk * heads, chunk * heads), BF16),
        pltpu.VMEM((chunk * heads, chunk * heads), BF16),
        pltpu.VMEM((chunk * 16, head), BF16),
        pltpu.VMEM((chunk * 16, head), BF16),
        pltpu.VMEM((chunk * heads, 2 * head), F32),
        pltpu.VMEM((chunk * heads, slots * kv), F32),
        pltpu.VMEM((chunk * heads, head), F32),
        pltpu.VMEM((batch * heads, slots * kv), F32),
        pltpu.VMEM((batch * 16, head), BF16),
        pltpu.VMEM((batch, head), F32),
        pltpu.VMEM((batch, head), F32),
        pltpu.VMEM((insts, chunk, width), BF16),
        pltpu.VMEM((insts, chunk // 2, width), BF16),
        pltpu.VMEM((insts, chunk // 2, width), BF16),
        pltpu.VMEM((insts, chunk // 2, width), BF16),
        pltpu.VMEM((2 * layers, batch, width), BF16),
        pltpu.SemaphoreType.DMA((layers, len(weights))),
        pltpu.SemaphoreType.DMA((layers, batch // BLK)),
        pltpu.SemaphoreType.DMA((layers, batch // BLK)),
        pltpu.SemaphoreType.DMA((3, insts)),
        pltpu.SemaphoreType.DMA((3, insts)),
    ]
    x_out, k_out, v_out = pl.pallas_call(
        functools.partial(step_kernel, chunk),
        out_shape=(jax.ShapeDtypeStruct(x_in.shape, BF16), pltpu.VMEM(flat, BF16), pltpu.VMEM(flat, BF16)),
        in_specs=[vmem] * 8 + [hbm] * 9,
        out_specs=(vmem, vmem, vmem),
        scratch_shapes=scratch,
        compiler_params=pltpu.CompilerParams(collective_id=0, has_side_effects=True, vmem_limit_bytes=28 * 2 ** 20),
        name="decode_step",
    )(x_in, seq_lens.reshape(1, batch), freq, g_attn, g_mlp, b_q, b_k, b_v, *weights, k_cache.reshape(flat), v_cache.reshape(flat))
    return x_out, k_out.reshape(k_cache.shape), v_out.reshape(v_cache.shape)


def solution(mesh):
    weight_col = P(None, None, "tp")
    weight_row = P(None, "tp", None)
    bias_col = P(None, "tp")
    cache_spec = P(None, "dp", None, "tp", None)
    in_specs = (P("dp", None), P("dp"), P(None, None), P(None, None), weight_col, bias_col, weight_col, bias_col, weight_col, bias_col, weight_row, weight_col, weight_col, weight_row, cache_spec, cache_spec)
    out_specs = (P("dp", None), cache_spec, cache_spec)
    return jax.shard_map(run_step, mesh=mesh, in_specs=in_specs, out_specs=out_specs, check_vma=False)
```

```python
import functools

import jax
import jax.numpy as jnp
import numpy as np
from jax import lax
from jax.experimental import pallas as pl
from jax.experimental.pallas import tpu as pltpu
from jax.sharding import PartitionSpec as P

ROPE_THETA = 1000000.0
EPS = 1e-6
F32 = jnp.float32
BF16 = jnp.bfloat16
MESH = pl.DeviceIdType.MESH
BLK = 16
STEP = 32


def dot(lhs, rhs):
    return jnp.dot(lhs, rhs, preferred_element_type=F32)


def dot_nt(lhs, rhs):
    return lax.dot_general(lhs, rhs, (((1,), (1,)), ((), ())), preferred_element_type=F32)


def one_hot(shape, hit):
    rows = lax.broadcasted_iota(jnp.int32, shape, 0)
    cols = lax.broadcasted_iota(jnp.int32, shape, 1)
    return jnp.where(hit(rows, cols), 1.0, 0.0).astype(BF16)


def step_kernel(chunk, x_in, lens_in, freq_in, g_attn_in, g_mlp_in, bq_in, bk_in, bv_in,
                wq_hbm, wk_hbm, wv_hbm, wo_hbm, wg_hbm, wu_hbm, wd_hbm, kc_hbm, vc_hbm,
                xo_ref, sum_ref, kn_ref, vn_ref, kv_out,
                x_ref, lens_ref, freq_ref, g_attn_ref, g_mlp_ref, bq_ref, bk_ref, bv_ref,
                wq, wk, wv, wo, wg, wu, wd,
                gather, ungather, gather_kv, pairs, qlhs, scores, fresh, rows_out, limit, cos_t, sin_t,
                part, recv_a, mid, recv_b, recv_d, xs,
                s_sem, w_sem, k_sem, v_sem, send_sem, recv_sem):
    ko_ref, vo_ref = kv_out.at[0], kv_out.at[1]
    layers, batch, slots2, head = kv_out.shape[1:]
    heads = wq.shape[2] // head
    kv = wk.shape[2] // head
    group = heads // kv
    n_chunks = batch // chunk
    half = chunk // 2
    blocks = chunk // BLK
    tp = lax.axis_index("tp")
    core = lax.rem(tp, 2)
    chip = tp // 2
    core_peer = {"tp": chip * 2 + (1 - core)}
    chip_peer = {"tp": (1 - chip) * 2 + core}

    weights = ((wq_hbm, wq), (wk_hbm, wk), (wv_hbm, wv), (wo_hbm, wo), (wg_hbm, wg), (wu_hbm, wu), (wd_hbm, wd))

    def weight_copy(layer, idx):
        src, dst = weights[idx]
        return pltpu.make_async_copy(src.at[layer], dst.at[layer], w_sem.at[layer, idx])

    def cache_copy(src, dst, sem, layer, blk):
        return pltpu.make_async_copy(src.at[layer, pl.ds(blk * BLK, BLK)], dst.at[layer, pl.ds(blk * BLK, BLK)], sem.at[layer, blk])

    def start_weights(layer, idxs):
        for idx in idxs:
            weight_copy(layer, idx).start()

    def wait_weights(layer, idxs):
        for idx in idxs:
            weight_copy(layer, idx).wait()

    def start_cache(layer, c):
        for src, dst, sem in ((kc_hbm, ko_ref, k_sem), (vc_hbm, vo_ref, v_sem)):
            @pl.loop(0, blocks)
            def _(i):
                cache_copy(src, dst, sem, layer, c * blocks + i).start()

    smalls = ((x_in, x_ref), (lens_in, lens_ref), (freq_in, freq_ref), (g_attn_in, g_attn_ref), (g_mlp_in, g_mlp_ref),
              (bq_in, bq_ref), (bk_in, bk_ref), (bv_in, bv_ref))
    for i, (src, dst) in enumerate(smalls):
        pltpu.make_async_copy(src, dst, s_sem.at[i]).start()
    start_weights(0, (0, 1, 2))
    start_cache(0, 0)

    barrier = pltpu.get_barrier_semaphore()
    for peer in (core_peer, chip_peer):
        pl.semaphore_signal(barrier, inc=1, device_id=peer, device_id_type=MESH)

    gather[...] = one_hot(gather.shape, lambda r, c: c == (r % heads) * chunk + r // heads)
    ungather[...] = one_hot(ungather.shape, lambda r, c: r == (c % heads) * chunk + c // heads)
    gather_kv[...] = one_hot(gather_kv.shape, lambda r, c: c == (r % heads) // group * chunk + r // heads)
    pairs[...] = one_hot(pairs.shape, lambda r, c: c == (r % kv) * chunk + r // kv)
    for i, (src, dst) in enumerate(smalls):
        pltpu.make_async_copy(src, dst, s_sem.at[i]).wait()
    lens = lens_ref[...].astype(F32)
    sq = (batch, batch)
    diag = lax.broadcasted_iota(jnp.int32, sq, 0) == lax.broadcasted_iota(jnp.int32, sq, 1)
    len_col = jnp.sum(jnp.where(diag, jnp.broadcast_to(lens, sq), 0.0), axis=1, keepdims=True)
    len_cols = jnp.broadcast_to(len_col, (batch, head))
    angles = len_cols * freq_ref[...]
    cos_t[...] = jnp.cos(angles)
    lane = lax.broadcasted_iota(jnp.int32, (batch, head), 1)
    sine = jnp.sin(angles)
    sin_t[...] = jnp.where(lane < head // 2, -sine, sine)
    len_bf = len_cols.astype(BF16)
    row_len = dot(one_hot((batch * heads, batch), lambda r, c: c == r // heads), len_bf)
    row_len = jnp.concatenate([row_len] * (slots2 // head), axis=1)
    lim_shape = (batch * heads, slots2)
    q_head = lax.broadcasted_iota(jnp.int32, lim_shape, 0) % heads
    own = lax.broadcasted_iota(jnp.int32, lim_shape, 1) % kv == q_head // group
    limit[...] = jnp.where(own, row_len, -1.0)

    def rms_norm(x_bf, gain_ref, layer):
        x = x_bf.astype(F32)
        mean_sq = jnp.mean(x * x, axis=-1, keepdims=True)
        return (x * lax.rsqrt(mean_sq + EPS) * gain_ref[pl.ds(layer, 1), :].astype(F32)).astype(BF16)

    def read_x(stage, c):
        src = x_ref if stage == 0 else xs.at[stage - 1]
        return src[pl.ds(c * chunk, chunk), :]

    def qkv(layer, c):
        h = rms_norm(read_x(2 * layer, c), g_attn_ref, layer)
        cos = cos_t[pl.ds(c * chunk, chunk), :]
        sin = sin_t[pl.ds(c * chunk, chunk), :]

        def rope(vec):
            return (vec * cos + pltpu.roll(vec, head // 2, 1) * sin).astype(BF16)

        def split(mat, n):
            return [mat[:, i * head:(i + 1) * head] for i in range(n)]

        q = dot(h, wq[layer]) + bq_ref[pl.ds(layer, 1), :].astype(F32)
        k = dot(h, wk[layer]) + bk_ref[pl.ds(layer, 1), :].astype(F32)
        v = dot(h, wv[layer]) + bv_ref[pl.ds(layer, 1), :].astype(F32)
        q_stack = jnp.concatenate([rope(m) for m in split(q, heads)], axis=0)
        k_stack = jnp.concatenate([rope(m) for m in split(k, kv)], axis=0)
        v_stack = jnp.concatenate([m.astype(BF16) for m in split(v, kv)], axis=0)
        kn_ref[layer, pl.ds(c * kv * chunk, kv * chunk), :] = dot(pairs[...], k_stack).astype(BF16)
        vn_ref[layer, pl.ds(c * kv * chunk, kv * chunk), :] = dot(pairs[...], v_stack).astype(BF16)
        q_rows = dot(gather[...], q_stack)
        k_rows = dot(gather_kv[...], k_stack)
        fresh[...] = dot(gather_kv[...], v_stack)
        first = lax.broadcasted_iota(jnp.int32, q_rows.shape, 0) % (2 * heads) < heads
        qlhs[...] = jnp.concatenate([jnp.where(first, q_rows, 0.0), jnp.where(first, 0.0, q_rows)], axis=1)
        return jnp.sum(q_rows * k_rows, axis=-1, keepdims=True)

    def by_pairs(src, dst, sem, layer, c, one_pair):
        @pl.loop(0, chunk // STEP)
        def _(i):
            for j in range(STEP // BLK):
                cache_copy(src, dst, sem, layer, c * blocks + i * (STEP // BLK) + j).wait()
            for pair in range(STEP // 2):
                b = i * STEP + 2 * pair
                row = c * chunk + b
                rhs = jnp.concatenate([dst[layer, row], dst[layer, row + 1]], axis=1)
                one_pair(pl.ds(pl.multiple_of(b * heads, 2 * heads), 2 * heads), rhs)

    def attn_scores(layer, c):
        def one_pair(rows, rhs):
            scores[rows, :] = dot_nt(qlhs[rows, :].astype(BF16), rhs)

        by_pairs(kc_hbm, ko_ref, k_sem, layer, c, one_pair)

    def attn_softmax(c, new_score):
        s = scores[...] * (head ** -0.5)
        s_new = new_score * (head ** -0.5)
        slot = (lax.broadcasted_iota(jnp.int32, s.shape, 1) // kv).astype(F32)
        s = jnp.where(slot < limit[pl.ds(c * chunk * heads, chunk * heads), :], s, -1e30)
        top = jnp.maximum(jnp.max(s, axis=-1, keepdims=True), s_new)
        e = jnp.exp(s - top)
        e_new = jnp.exp(s_new - top)
        total = jnp.sum(e, axis=-1, keepdims=True) + e_new
        scores[...] = e / total
        fresh[...] = fresh[...] * (e_new / total).astype(BF16).astype(F32)

    def attn_values(layer, c):
        def one_pair(rows, rhs):
            out = dot(scores[rows, :].astype(BF16), rhs)
            first = lax.broadcasted_iota(jnp.int32, (2 * heads, head), 0) < heads
            rows_out[rows, :] = jnp.where(first, out[:, :head], out[:, head:]) + fresh[rows, :]

        by_pairs(vc_hbm, vo_ref, v_sem, layer, c, one_pair)

    def attn_project(layer, c):
        stacked = dot(ungather[...], rows_out[...].astype(BF16)).astype(BF16)
        attn = jnp.concatenate([stacked[i * chunk:(i + 1) * chunk, :] for i in range(heads)], axis=1)
        part[2 * layer * n_chunks + c] = dot(attn, wo[layer]).astype(BF16)

    def mlp(layer, c):
        h = rms_norm(read_x(2 * layer + 1, c), g_mlp_ref, layer)
        act = (jax.nn.silu(dot(h, wg[layer])) * dot(h, wu[layer])).astype(BF16)
        part[(2 * layer + 1) * n_chunks + c] = dot(act, wd[layer]).astype(BF16)

    last = 2 * layers - 1
    mine = pl.ds(pl.multiple_of(core * half, half), half)
    other = pl.ds(pl.multiple_of((1 - core) * half, half), half)

    def send(hop, inst, src, dst, peer):
        return pltpu.make_async_remote_copy(src_ref=src, dst_ref=dst, send_sem=send_sem.at[hop, inst], recv_sem=recv_sem.at[hop, inst],
                                            device_id=peer, device_id_type=MESH)

    def hop_a(s, c):
        inst = s * n_chunks + c
        return send(0, inst, part.at[inst, other], recv_a.at[inst], core_peer)

    def hop_b(s, c):
        inst = s * n_chunks + c
        return send(1, inst, mid.at[inst], recv_b.at[inst], chip_peer)

    def hop_c(s, c):
        rows = pl.ds(pl.multiple_of(c * chunk + core * half, half), half)
        return send(2, s * n_chunks + c, xs.at[s, rows], xs.at[s, rows], core_peer)

    def hop_d(s, c):
        inst = s * n_chunks + c
        return send(3, inst, part.at[inst], recv_d.at[c], core_peer)

    def sum_start(s, c):
        (hop_d if s == last else hop_a)(s, c).start()

    def chip_sum(c):
        inst = last * n_chunks + c
        hop_d(last, c).wait_recv()
        sum_ref[pl.ds(c * chunk, chunk), :] = (part[inst].astype(F32) + recv_d[c].astype(F32)).astype(BF16)

    def sum_cross(s, c):
        inst = s * n_chunks + c
        hop_a(s, c).wait_recv()
        mid[inst] = (part[inst, mine, :].astype(F32) + recv_a[inst].astype(F32)).astype(BF16)
        hop_b(s, c).start()

    def sum_share(s, c):
        inst = s * n_chunks + c
        hop_b(s, c).wait_recv()
        rows = pl.ds(pl.multiple_of(c * chunk + core * half, half), half)
        before = (x_ref if s == 0 else xs.at[s - 1])[rows, :]
        total = mid[inst].astype(F32) + recv_b[inst].astype(F32)
        xs[s, rows, :] = (before.astype(F32) + total).astype(BF16)
        hop_c(s, c).start()

    def sum_end(s, c):
        hop_c(s, c).wait_recv()

    def flow(layer):
        s = 2 * layer
        wait_weights(layer, (0, 1, 2))
        if layer == 0:
            start_weights(0, (3,))
            start_cache(0, 1)
        else:
            sum_end(s - 1, 0)
        new_score = qkv(layer, 0)
        attn_scores(layer, 0)
        if layer > 0:
            sum_share(s - 1, 1)
        attn_softmax(0, new_score)
        attn_values(layer, 0)
        wait_weights(layer, (3,))
        attn_project(layer, 0)
        if layer == 0:
            pl.semaphore_wait(barrier, 2)
        sum_start(s, 0)
        if layer == 0:
            start_weights(0, (4, 5, 6))
            start_weights(1, (0, 1, 2))
            start_cache(1, 0)
        else:
            sum_end(s - 1, 1)
        new_score = qkv(layer, 1)
        sum_cross(s, 0)
        attn_scores(layer, 1)
        attn_softmax(1, new_score)
        attn_values(layer, 1)
        attn_project(layer, 1)
        sum_start(s, 1)
        if layer == 0:
            start_cache(1, 1)
            start_weights(1, (3, 4, 5, 6))
        sum_share(s, 0)
        sum_cross(s, 1)
        wait_weights(layer, (4, 5, 6))
        sum_end(s, 0)
        mlp(layer, 0)
        sum_start(s + 1, 0)
        sum_share(s, 1)
        if s + 1 < last:
            sum_cross(s + 1, 0)
        sum_end(s, 1)
        mlp(layer, 1)
        sum_start(s + 1, 1)
        if s + 1 < last:
            sum_cross(s + 1, 1)
            sum_share(s + 1, 0)
        else:
            chip_sum(0)
            xo_ref[...] = xs[last - 1]
            chip_sum(1)

    for layer in range(layers):
        flow(layer)
    for s in range(last + 1):
        for c in range(n_chunks):
            for hop in (hop_d,) if s == last else (hop_a, hop_b, hop_c):
                hop(s, c).wait_send()


def write_kernel(lens_ref, kv_ref, kn_ref, vn_ref, ko_hbm, vo_hbm, sem, row_sem):
    k_ref, v_ref = kv_ref.at[0], kv_ref.at[1]
    layers, batch = kv_ref.shape[1:3]
    sides = ((k_ref, kn_ref, ko_hbm), (v_ref, vn_ref, vo_hbm))
    blocks = batch // BLK

    def copy(side, layer, blk):
        src, _, dst = sides[side]
        rows = pl.ds(blk * BLK, BLK)
        return pltpu.make_async_copy(src.at[layer, rows], dst.at[layer, rows], sem.at[side, layer, blk])

    for layer in range(layers):
        for side in range(2):
            @pl.loop(0, blocks)
            def _(blk):
                copy(side, layer, blk).start()

    for layer in range(layers):
        for side in range(2):
            _, new, dst = sides[side]

            @pl.loop(0, blocks)
            def _(blk):
                copy(side, layer, blk).wait()
                for i in range(BLK):
                    b = blk * BLK + i
                    pltpu.make_async_copy(new.at[layer, b], dst.at[layer, b, lens_ref[b]], row_sem.at[side]).start()

    for side in range(2):
        _, new, dst = sides[side]
        pltpu.make_async_copy(new, dst.at[:, :, 0], row_sem.at[side]).wait()


def run_step(x_in, seq_lens, g_attn, g_mlp, w_q, b_q, w_k, b_k, w_v, b_v, w_o, w_gate, w_up, w_down, k_cache, v_cache):
    layers, batch, slots, kv, head = k_cache.shape
    width = x_in.shape[1]
    heads = w_q.shape[2] // head
    chunk = batch // 2
    flat = (layers, batch, slots * kv, head)
    exponent = -2.0 * (np.arange(head) % (head // 2)) / head
    freq = jnp.asarray((ROPE_THETA ** exponent)[None, :], F32)
    insts = 2 * layers * 2
    vmem = pl.BlockSpec(memory_space=pltpu.VMEM)
    hbm = pl.BlockSpec(memory_space=pl.ANY)
    smalls = (x_in, seq_lens.reshape(1, batch), freq, g_attn, g_mlp, b_q, b_k, b_v)
    weights = (w_q, w_k, w_v, w_o, w_gate, w_up, w_down)
    rows = chunk * heads
    half = chunk // 2
    scratch = [pltpu.VMEM(a.shape, a.dtype) for a in smalls + weights]
    scratch += [
        pltpu.VMEM((rows, rows), BF16),
        pltpu.VMEM((rows, rows), BF16),
        pltpu.VMEM((rows, kv * chunk), BF16),
        pltpu.VMEM((kv * chunk, kv * chunk), BF16),
        pltpu.VMEM((rows, 2 * head), F32),
        pltpu.VMEM((rows, slots * kv), F32),
        pltpu.VMEM((rows, head), F32),
        pltpu.VMEM((rows, head), F32),
        pltpu.VMEM((batch * heads, slots * kv), F32),
        pltpu.VMEM((batch, head), F32),
        pltpu.VMEM((batch, head), F32),
        pltpu.VMEM((insts, chunk, width), BF16),
        pltpu.VMEM((insts, half, width), BF16),
        pltpu.VMEM((insts, half, width), BF16),
        pltpu.VMEM((insts, half, width), BF16),
        pltpu.VMEM((2, chunk, width), BF16),
        pltpu.VMEM((2 * layers - 1, batch, width), BF16),
        pltpu.SemaphoreType.DMA((len(smalls),)),
        pltpu.SemaphoreType.DMA((layers, len(weights))),
        pltpu.SemaphoreType.DMA((layers, batch // BLK)),
        pltpu.SemaphoreType.DMA((layers, batch // BLK)),
        pltpu.SemaphoreType.DMA((4, insts)),
        pltpu.SemaphoreType.DMA((4, insts)),
    ]
    fresh = pltpu.VMEM((layers, batch * kv, head), BF16)
    x_mid, share, k_new, v_new, held_kv = pl.pallas_call(
        functools.partial(step_kernel, chunk),
        out_shape=(pltpu.VMEM(x_in.shape, BF16), pltpu.VMEM(x_in.shape, BF16), fresh, fresh, pltpu.VMEM((2,) + flat, BF16)),
        in_specs=[hbm] * 17,
        out_specs=(vmem,) * 5,
        scratch_shapes=scratch,
        compiler_params=pltpu.CompilerParams(collective_id=0, has_side_effects=True, vmem_limit_bytes=26 * 2 ** 20),
        cost_estimate=pl.CostEstimate(flops=2 * 10 ** 10, bytes_accessed=5 * 10 ** 7, transcendentals=0),
        name="decode_step",
    )(*smalls, *weights, k_cache.reshape(flat), v_cache.reshape(flat))

    ranks = lax.axis_size("tp")
    other_share = lax.ppermute(share, "tp", [(i, (i + ranks // 2) % ranks) for i in range(ranks)])
    new_rows = (layers, batch, kv, head)
    held = (held_kv.reshape((2,) + k_cache.shape), k_new.reshape(new_rows), v_new.reshape(new_rows))
    cache_out = jax.ShapeDtypeStruct(k_cache.shape, BF16)
    k_out, v_out = pl.pallas_call(
        write_kernel,
        out_shape=(cache_out, cache_out),
        in_specs=[pl.BlockSpec(memory_space=pltpu.SMEM)] + [vmem] * 3,
        out_specs=(hbm, hbm),
        scratch_shapes=[pltpu.SemaphoreType.DMA((2, layers, batch // BLK)), pltpu.SemaphoreType.DMA((2,))],
        compiler_params=pltpu.CompilerParams(vmem_limit_bytes=2 ** 20),
        cost_estimate=pl.CostEstimate(flops=2 * 10 ** 10, bytes_accessed=4 * 10 ** 7, transcendentals=0),
        name="write_caches",
    )(seq_lens, *held)
    x_out = (x_mid.astype(F32) + (share.astype(F32) + other_share.astype(F32))).astype(BF16)
    return x_out, k_out, v_out


def solution(mesh):
    weight_col = P(None, None, "tp")
    weight_row = P(None, "tp", None)
    bias_col = P(None, "tp")
    cache_spec = P(None, "dp", None, "tp", None)
    in_specs = (P("dp", None), P("dp"), P(None, None), P(None, None), weight_col, bias_col, weight_col, bias_col, weight_col, bias_col, weight_row, weight_col, weight_col, weight_row, cache_spec, cache_spec)
    out_specs = (P("dp", None), cache_spec, cache_spec)
    return jax.shard_map(run_step, mesh=mesh, in_specs=in_specs, out_specs=out_specs, check_vma=False)
```
